32 devices in a mesh: lev: 2 (over core), wa: 16 (over z, y, x).
Axes of the slice: x: 2, y: 2, z: 4, core: 2. Of those that a mesh axis runs over, the one named last changes fastest.
Arguments:
- spectral: bfloat16 [1280, 1280, 2, 64], P('wa', None, None, 'lev'), parts along dimension 3, may hold values from -0.15625 to 0.15625
- legendre: bfloat16 [1280, 1280, 48], P('wa'), may hold values from -0.15625 to 0.15625
- wavenumber: int32 [1280], P('wa'), may hold values from 0 to 1279, each once
Outputs:
- grid: float32 [96, 2560, 64], P('wa', None, 'lev'), parts along dimension 2
The draws below stay inside these ranges and needn't reach their ends.
There are 2 independent parts, one for each index of `lev`. The reference program is written for one: setup_inputs(seed, part) draws one part's arguments, and reference() takes and returns one part's arrays. A program takes and returns all parts, laid end to end along the dimension named above; an argument that names none is the same for every part. Nothing has to cross between parts.
Inputs may be any that keep to these rules, and one draw needn't show every extreme that they name: wavenumber names every number of 0 to 1279 exactly once; slot k of spectral and legendre belongs to wavenumber[k].
All inputs are finite; a program needn't handle non-finite values.
Results may differ from the reference program's by a relative error of at most 0.0003.
Values sent between devices are 32-bit elements.
A program may use at most 128 MiB of HBM per device.

```python
import jax
import jax.numpy as jnp
from jax import lax

TRUNC = 1279
NLON = 2560
LEVELS = 32
WAVES = 1280
NORTH = 48


def level_of(stream_key, dims, shards, low, high):
    def one(axis_at, shards_of):
        heights = jax.random.uniform(jax.random.fold_in(jax.random.fold_in(stream_key, 6), axis_at), (shards_of,), jnp.float32, low / len(shards), high / len(shards))
        return jnp.repeat(jnp.exp(heights), dims[axis_at] // shards_of).reshape((-1,) + (1,) * (len(dims) - axis_at - 1))

    factor_of = one(*shards[0])
    for cut in shards[1:]:
        factor_of = factor_of * one(*cut)
    return factor_of


def scatter_about(rng, shape, deviation, limit, cuts=(), kind=jnp.bfloat16):
    values = deviation * jax.random.normal(rng, shape, jnp.float32)
    if cuts:
        values = values * level_of(rng, shape, cuts, -0.22, 0.18)
    return jnp.clip(values, -limit, limit).astype(kind)


def setup_inputs(seed: int = 0, part: int = 0) -> dict:
    streams_of = jax.random.split(jax.random.key(seed), 4)
    own_keys = jax.random.split(jax.random.fold_in(streams_of[3], part), 4)
    return {
        "spectral": scatter_about(own_keys[0], (WAVES, WAVES, 2, LEVELS), (TRUNC + 1) ** -0.5, 0.15625, ((0, 16),)),
        "legendre": scatter_about(streams_of[1], (WAVES, WAVES, NORTH), (TRUNC + 1) ** -0.5, 0.15625, ((0, 16),)),
        "wavenumber": jax.random.permutation(streams_of[2], TRUNC + 1).astype(jnp.int32),
    }


def reference(spectral, legendre, wavenumber):
    degrees = spectral.shape[1]
    levels = spectral.shape[3]
    row_index = jnp.arange(degrees, dtype=jnp.int32)

    def one_slot(slot_item):
        rows_table, coeffs, slot_wave = slot_item
        coeff_rows = coeffs.reshape(degrees, 2 * levels)
        kept = jnp.where((row_index >= slot_wave)[:, None], coeff_rows, jnp.zeros_like(coeff_rows))
        flipped = jnp.where(((row_index - slot_wave) % 2 == 0)[:, None], kept, -kept)
        north_sums = jnp.dot(rows_table.T, kept, preferred_element_type=jnp.float32)
        south_sums = jnp.dot(rows_table.T, flipped, preferred_element_type=jnp.float32)
        return jnp.concatenate([north_sums, south_sums[::-1]], 0)

    fourier = lax.map(one_slot, (legendre, spectral, wavenumber))
    real_part = fourier[..., :levels]
    imag_part = fourier[..., levels:] * (wavenumber != 0).astype(fourier.dtype)[:, None, None]
    complex_coeffs = lax.complex(real_part, imag_part)
    spectrum = jnp.zeros((NLON // 2 + 1,) + real_part.shape[1:], complex_coeffs.dtype)
    spectrum = spectrum.at[wavenumber].set(complex_coeffs)
    gridded = jnp.fft.irfft(spectrum, n=NLON, axis=0) * NLON
    return jnp.transpose(gridded, (1, 0, 2)).astype(jnp.float32)
```

```python
import functools
import math

import jax
import jax.numpy as jnp
from jax import lax
from jax.experimental import pallas as pl
from jax.experimental.pallas import tpu as pltpu
from jax.sharding import PartitionSpec as P

NLON = 2560
PAIRS = 8
TILE = 256


def exchange_kernel(
    n, chunks, real_pairs, north,
    wave_smem, wave_row, spectral, legendre,
    recv, wave_all,
    send, send_sem, recv_sem, wave_send, wave_recv, own_sem,
):
    me = lax.axis_index("wa")
    step = pl.program_id(0)
    half = n // 2
    block = 2 * north // n * PAIRS

    def rows_for(dst):
        south = dst // half
        slab = (1 - south) * dst + south * (half + n - 1 - dst)
        return pl.ds(pl.multiple_of(slab * block, 8), block)

    def wave_copy(i):
        dst = lax.rem(me + i, n)
        return pltpu.make_async_remote_copy(
            src_ref=wave_row, dst_ref=wave_all.at[me],
            send_sem=wave_send.at[dst], recv_sem=wave_recv.at[me],
            device_id={"wa": dst}, device_id_type=pl.DeviceIdType.MESH,
        )

    def data_copy(c, i):
        dst = lax.rem(me + i, n)
        return pltpu.make_async_remote_copy(
            src_ref=send.at[c, rows_for(dst)], dst_ref=recv.at[c, me],
            send_sem=send_sem.at[c, dst], recv_sem=recv_sem.at[c, me],
            device_id={"wa": dst}, device_id_type=pl.DeviceIdType.MESH,
        )

    def data_arrival(c, i):
        src = lax.rem(me + i, n)
        return pltpu.make_async_remote_copy(
            src_ref=send.at[c, rows_for(src)], dst_ref=recv.at[c, src],
            send_sem=send_sem.at[c, src], recv_sem=recv_sem.at[c, src],
            device_id={"wa": src}, device_id_type=pl.DeviceIdType.MESH,
        )

    def wave_arrival(i):
        src = lax.rem(me + i, n)
        return pltpu.make_async_remote_copy(
            src_ref=wave_row, dst_ref=wave_all.at[src],
            send_sem=wave_send.at[src], recv_sem=wave_recv.at[src],
            device_id={"wa": src}, device_id_type=pl.DeviceIdType.MESH,
        )

    def own_copy(c):
        return pltpu.make_async_copy(send.at[c, rows_for(me)], recv.at[c, me], own_sem.at[c])

    own_wave = pltpu.make_async_copy(wave_row, wave_all.at[me], own_sem.at[chunks])

    @pl.when(step == 0)
    def _():
        barrier = pltpu.get_barrier_semaphore()

        def greet(i, carry):
            pl.semaphore_signal(
                barrier, inc=1, device_id={"wa": lax.rem(me + i, n)},
                device_id_type=pl.DeviceIdType.MESH,
            )
            return carry

        lax.fori_loop(1, n, greet, 0)
        pl.semaphore_wait(barrier, n - 1)

        def send_wave(i, carry):
            wave_copy(i).start()
            return carry

        lax.fori_loop(1, n, send_wave, 0)
        own_wave.start()

    degrees = spectral.shape[-1]
    columns = spectral.shape[1]
    index = lax.broadcasted_iota(jnp.int32, (1, degrees), 1)
    lane = lax.broadcasted_iota(jnp.int32, (1, 2 * columns), 1)

    def sums_of(slot):
        offset = index - wave_smem[step * 2 * real_pairs + slot]
        keep = jnp.where(offset >= 0, 1.0, 0.0)
        flip = jnp.where(offset % 2 == 0, keep, -keep)
        coeff = spectral[slot]
        both = jnp.concatenate(
            [coeff * keep.astype(coeff.dtype), coeff * flip.astype(coeff.dtype)], 0
        )
        return lax.dot_general(
            legendre[slot], both, (((1,), (1,)), ((), ())), preferred_element_type=jnp.float32
        )

    for p in range(PAIRS):
        if p < real_pairs:
            first = sums_of(2 * p)
            second = sums_of(2 * p + 1)
            first_turned = pltpu.roll(first, columns, 1)
            second_turned = pltpu.roll(second, columns, 1)
            north_rows = jnp.where(lane < columns, first, second_turned)
            south_rows = jnp.where(lane < columns, first_turned, second)
        else:
            north_rows = south_rows = jnp.zeros((north, 2 * columns), jnp.float32)
        send[step, pl.ds(p, north, stride=PAIRS), :] = north_rows
        send[step, pl.ds(north * PAIRS + p, north, stride=PAIRS), :] = south_rows

    def send_data(i, carry):
        data_copy(step, i).start()
        return carry

    lax.fori_loop(1, n, send_data, 0)
    own_copy(step).start()

    @pl.when(step == chunks - 1)
    def _():
        own_wave.wait()

        def finish_wave(i, carry):
            wave_copy(i).wait_send()
            wave_arrival(i).wait_recv()
            return carry

        lax.fori_loop(1, n, finish_wave, 0)
        for c in range(chunks):
            own_copy(c).wait()

            def finish(i, carry, c=c):
                data_copy(c, i).wait_send()
                data_arrival(c, i).wait_recv()
                return carry

            lax.fori_loop(1, n, finish, 0)


def cos_sin(turns):
    quarter = jnp.floor(turns * (4.0 / NLON) + 0.5)
    x = (turns - quarter * (NLON // 4)) * (2.0 * math.pi / NLON)
    y = x * x
    s = x * (1.0 + y * (-1 / 6 + y * (1 / 120 + y * (-1 / 5040 + y * (1 / 362880)))))
    c = 1.0 + y * (-1 / 2 + y * (1 / 24 + y * (-1 / 720 + y * (1 / 40320 - y * (1 / 3628800)))))
    which = quarter.astype(jnp.int32) & 3
    odd = (which & 1) == 1
    cos_out = jnp.where(odd, s, c)
    sin_out = jnp.where(odd, c, s)
    cos_out = jnp.where((which == 1) | (which == 2), -cos_out, cos_out)
    sin_out = jnp.where(which >= 2, -sin_out, sin_out)
    return cos_out, sin_out


def synthesis_kernel(south_ref, wave_ref, data, out, hi, lo, cos_now, sin_now, table_hi, table_lo):
    step = pl.program_id(0)
    groups, rows, pairs, lanes = data.shape
    depth = groups * pairs
    levels = lanes // 4

    @pl.when(step == 0)
    def _():
        lane = lax.broadcasted_iota(jnp.int32, (1, lanes), 1)
        sign = jnp.where((lane // levels) % 2 == 1, -1.0, 1.0)
        weight = jnp.where(wave_ref[...] == 0.0, 1.0, 2.0)
        scale = jnp.where(lane < 2 * levels, weight[:depth], weight[depth:]) * sign
        south = south_ref[0]
        for row in range(rows):
            source = row + south * (rows - 1 - 2 * row)
            values = data[:, source].reshape(depth, lanes) * scale
            turned = values.T
            for g in range(4):
                part = turned[g * levels:(g + 1) * levels]
                part_hi = part.astype(jnp.bfloat16)
                place = (slice(row * levels, (row + 1) * levels), slice(g * depth, (g + 1) * depth))
                hi[place] = part_hi
                lo[place] = (part - part_hi.astype(jnp.float32)).astype(jnp.bfloat16)
        position = lax.broadcasted_iota(jnp.int32, (1, TILE), 1).astype(jnp.float32)

        def begin(i, carry):
            at = pl.ds(pl.multiple_of(i * 16, 16), 16)
            c, s = cos_sin(wave_ref[at, :] * position)
            cos_now[at, :] = c
            sin_now[at, :] = s
            return carry

        lax.fori_loop(0, 2 * depth // 16, begin, 0, unroll=2)

    for sp in range(2):
        def fill(i, carry, sp=sp):
            at = pl.ds(pl.multiple_of(sp * depth + i * 16, 16), 16)
            c = cos_now[at, :]
            s = sin_now[at, :]
            turn_c, turn_s = cos_sin(wave_ref[at, :] * float(TILE))
            for values, part in ((c, 0), (s, 1)):
                to = pl.ds(pl.multiple_of((2 * sp + part) * depth + i * 16, 16), 16)
                top = values.astype(jnp.bfloat16)
                table_hi[to, :] = top
                table_lo[to, :] = (values - top.astype(jnp.float32)).astype(jnp.bfloat16)
            cos_now[at, :] = c * turn_c - s * turn_s
            sin_now[at, :] = s * turn_c + c * turn_s
            return carry

        lax.fori_loop(0, depth // 16, fill, 0, unroll=4)
    high = table_hi[...]
    total = jnp.dot(hi[...], high, preferred_element_type=jnp.float32)
    total += jnp.dot(lo[...], high, preferred_element_type=jnp.float32)
    total += jnp.dot(hi[...], table_lo[...], preferred_element_type=jnp.float32)
    out[...] = total.reshape(out.shape)


def on_device(spectral, legendre, wavenumber):
    slots, degrees, _, levels = spectral.shape
    north = legendre.shape[2]
    n = lax.axis_size("wa")
    rows = 2 * north // n
    pairs = slots // 2
    real_pairs = min(pairs, PAIRS)
    chunks = pairs // real_pairs
    coeff = jnp.transpose(spectral, (0, 2, 3, 1)).reshape(slots, 2 * levels, degrees)
    values = jnp.transpose(legendre, (0, 2, 1))
    wave_row = jnp.broadcast_to(jnp.pad(wavenumber, (0, 128 - slots))[None], (8, 128))
    block = rows * PAIRS
    per_step = 2 * real_pairs
    recv, wave_all = pl.pallas_call(
        functools.partial(exchange_kernel, n, chunks, real_pairs, north),
        grid=(chunks,),
        out_shape=(
            jax.ShapeDtypeStruct((chunks, n, block, 4 * levels), jnp.float32),
            jax.ShapeDtypeStruct((n, 8, 128), jnp.int32),
        ),
        in_specs=[
            pl.BlockSpec(memory_space=pltpu.SMEM),
            pl.BlockSpec(memory_space=pltpu.VMEM),
            pl.BlockSpec((per_step, 2 * levels, degrees), lambda i: (i, 0, 0)),
            pl.BlockSpec((per_step, north, degrees), lambda i: (i, 0, 0)),
        ],
        out_specs=(pl.BlockSpec(memory_space=pl.ANY), pl.BlockSpec(memory_space=pl.ANY)),
        scratch_shapes=[
            pltpu.VMEM((chunks, 2 * north * PAIRS, 4 * levels), jnp.float32),
            pltpu.SemaphoreType.DMA((chunks, n)),
            pltpu.SemaphoreType.DMA((chunks, n)),
            pltpu.SemaphoreType.DMA((n,)),
            pltpu.SemaphoreType.DMA((n,)),
            pltpu.SemaphoreType.DMA((chunks + 1,)),
        ],
        compiler_params=pltpu.CompilerParams(
            collective_id=0, has_side_effects=True, dimension_semantics=("arbitrary",)
        ),
    )(wavenumber, wave_row, coeff, values)
    waves = wave_all[:, 0, :slots].reshape(n, chunks, real_pairs, 2)
    waves = jnp.pad(waves, ((0, 0), (0, 0), (0, PAIRS - real_pairs), (0, 0)))
    depth = chunks * n * PAIRS
    waves = jnp.transpose(waves, (3, 1, 0, 2)).reshape(2 * depth, 1).astype(jnp.float32)
    south = (lax.axis_index("wa") >= n // 2).astype(jnp.int32).reshape(1)
    grid = pl.pallas_call(
        synthesis_kernel,
        grid=(NLON // TILE,),
        out_shape=jax.ShapeDtypeStruct((rows, levels, NLON), jnp.float32),
        in_specs=[
            pl.BlockSpec(memory_space=pltpu.SMEM),
            pl.BlockSpec((2 * depth, 1), lambda i: (0, 0)),
            pl.BlockSpec((chunks * n, rows, PAIRS, 4 * levels), lambda i: (0, 0, 0, 0)),
        ],
        out_specs=pl.BlockSpec((rows, levels, TILE), lambda i: (0, 0, i)),
        scratch_shapes=[
            pltpu.VMEM((rows * levels, 4 * depth), jnp.bfloat16),
            pltpu.VMEM((rows * levels, 4 * depth), jnp.bfloat16),
            pltpu.VMEM((2 * depth, TILE), jnp.float32),
            pltpu.VMEM((2 * depth, TILE), jnp.float32),
            pltpu.VMEM((4 * depth, TILE), jnp.bfloat16),
            pltpu.VMEM((4 * depth, TILE), jnp.bfloat16),
        ],
        compiler_params=pltpu.CompilerParams(dimension_semantics=("arbitrary",)),
    )(south, waves, recv.reshape(chunks * n, rows, PAIRS, 4 * levels))
    return jnp.transpose(grid, (0, 2, 1))


def solution(mesh):
    return jax.shard_map(
        on_device,
        mesh=mesh,
        in_specs=(P("wa", None, None, "lev"), P("wa", None, None), P("wa")),
        out_specs=P("wa", None, "lev"),
        check_vma=False,
    )
```

```python
import functools
import math

import jax
import jax.numpy as jnp
from jax import lax
from jax.experimental import pallas as pl
from jax.experimental.pallas import tpu as pltpu
from jax.sharding import PartitionSpec as P

NLON = 2560
PAIRS = 8
TILE = 256
LANES = 128


def cos_sin(turns):
    quarter = jnp.floor(turns * (4.0 / NLON) + 0.5)
    x = (turns - quarter * (NLON // 4)) * (2.0 * math.pi / NLON)
    y = x * x
    s = x * (1.0 + y * (-1 / 6 + y * (1 / 120 + y * (-1 / 5040 + y * (1 / 362880)))))
    c = 1.0 + y * (-1 / 2 + y * (1 / 24 + y * (-1 / 720 + y * (1 / 40320 - y * (1 / 3628800)))))
    which = quarter.astype(jnp.int32) & 3
    odd = (which & 1) == 1
    cos_out = jnp.where(odd, s, c)
    sin_out = jnp.where(odd, c, s)
    cos_out = jnp.where((which == 1) | (which == 2), -cos_out, cos_out)
    sin_out = jnp.where(which >= 2, -sin_out, sin_out)
    return cos_out, sin_out


def transform_kernel(
    n, chunks, real_pairs, north,
    wave_smem, spectral, legendre,
    out,
    send, recv, wave_row, wave_all, wave_columns, wave_rows,
    cos_hi, cos_lo, sin_hi, sin_lo, even, odd,
    send_sem, recv_sem, wave_send, wave_recv, own_sem,
):
    me = lax.axis_index("wa")
    step = pl.program_id(0)
    half = n // 2
    rows = 2 * north // n
    block = rows * PAIRS

    def rows_for(dst):
        south = dst // half
        slab = (1 - south) * dst + south * (half + n - 1 - dst)
        return pl.ds(pl.multiple_of(slab * block, 8), block)

    def wave_copy(peer, owner):
        return pltpu.make_async_remote_copy(
            src_ref=wave_row, dst_ref=wave_all.at[owner],
            send_sem=wave_send.at[peer], recv_sem=wave_recv.at[owner],
            device_id={"wa": peer}, device_id_type=pl.DeviceIdType.MESH,
        )

    def data_copy(c, peer, owner):
        return pltpu.make_async_remote_copy(
            src_ref=send.at[c, rows_for(peer)], dst_ref=recv.at[c, owner],
            send_sem=send_sem.at[c, peer], recv_sem=recv_sem.at[c, owner],
            device_id={"wa": peer}, device_id_type=pl.DeviceIdType.MESH,
        )

    def own_copy(c):
        return pltpu.make_async_copy(send.at[c, rows_for(me)], recv.at[c, me], own_sem.at[c])

    own_wave = pltpu.make_async_copy(wave_row, wave_all.at[me], own_sem.at[chunks])

    def each_peer(act):
        def one(i, carry):
            act(lax.rem(me + i, n))
            return carry

        lax.fori_loop(1, n, one, 0)

    @pl.when(step == 0)
    def _():
        barrier = pltpu.get_barrier_semaphore()
        each_peer(
            lambda peer: pl.semaphore_signal(
                barrier, inc=1, device_id={"wa": peer}, device_id_type=pl.DeviceIdType.MESH
            )
        )
        place = lax.broadcasted_iota(jnp.int32, wave_row.shape, 1)
        waves = jnp.zeros(wave_row.shape, jnp.int32)
        for slot in range(wave_smem.shape[0]):
            waves = jnp.where(place == slot, wave_smem[slot], waves)
        wave_row[...] = waves
        pl.semaphore_wait(barrier, n - 1)
        each_peer(lambda peer: wave_copy(peer, me).start())
        own_wave.start()

    degrees = spectral.shape[-1]
    columns = spectral.shape[1]
    levels = columns // 2
    index = lax.broadcasted_iota(jnp.int32, (1, degrees), 1)
    lane = lax.broadcasted_iota(jnp.int32, (1, 2 * columns), 1)

    def sums_of(slot):
        offset = index - wave_smem[step * 2 * real_pairs + slot]
        keep = jnp.where(offset >= 0, 1.0, 0.0)
        flip = jnp.where(offset % 2 == 0, keep, -keep)
        coeff = spectral[slot]
        both = jnp.concatenate(
            [coeff * keep.astype(coeff.dtype), coeff * flip.astype(coeff.dtype)], 0
        )
        return lax.dot_general(
            legendre[slot], both, (((1,), (1,)), ((), ())), preferred_element_type=jnp.float32
        )

    for p in range(PAIRS):
        if p < real_pairs:
            first = sums_of(2 * p)
            second = sums_of(2 * p + 1)
            first_turned = pltpu.roll(first, columns, 1)
            second_turned = pltpu.roll(second, columns, 1)
            north_rows = jnp.where(lane < columns, first, second_turned)
            south_rows = jnp.where(lane < columns, first_turned, second)
        else:
            north_rows = south_rows = jnp.zeros((north, 2 * columns), jnp.float32)
        send[step, pl.ds(p, north, stride=PAIRS), :] = north_rows
        send[step, pl.ds(north * PAIRS + p, north, stride=PAIRS), :] = south_rows

    each_peer(lambda peer: data_copy(step, peer, me).start())
    own_copy(step).start()

    @pl.when(step == chunks - 1)
    def _():
        own_wave.wait()
        each_peer(lambda peer: wave_copy(peer, peer).wait_recv())
        gathered = wave_all[:, 0, :].astype(jnp.float32)
        if n < LANES:
            gathered = jnp.concatenate([gathered, jnp.zeros((LANES - n, LANES), jnp.float32)], 0)
        wave_columns[...] = gathered.T
        for c in range(chunks):
            for sp in range(2):
                own = wave_columns[pl.ds(c * 2 * real_pairs + sp, PAIRS, stride=2), :]
                for owner in range(n):
                    to = ((2 * c + sp) * n + owner) * PAIRS
                    wave_rows[to:to + PAIRS, :] = jnp.broadcast_to(
                        own[:, owner:owner + 1], (PAIRS, LANES)
                    )
        position = lax.broadcasted_iota(jnp.int32, (1, LANES), 1).astype(jnp.float32)
        sin_tiles = sin_hi.shape[1] // LANES

        def fill(i, carry):
            at = pl.ds(pl.multiple_of(i * 16, 16), 16)
            waves = wave_rows[at, :]
            weight = jnp.where(waves == 0.0, 1.0, 2.0)
            c, s = cos_sin(waves * position)
            turn_c, turn_s = cos_sin(waves * float(LANES))
            c, s = c * weight, s * weight
            for tile in range(sin_tiles + 1):
                to = slice(tile * LANES, (tile + 1) * LANES)
                top = c.astype(jnp.bfloat16)
                cos_hi[at, to] = top
                cos_lo[at, to] = (c - top.astype(jnp.float32)).astype(jnp.bfloat16)
                if tile < sin_tiles:
                    top = s.astype(jnp.bfloat16)
                    sin_hi[at, to] = top
                    sin_lo[at, to] = (s - top.astype(jnp.float32)).astype(jnp.bfloat16)
                    c, s = c * turn_c - s * turn_s, s * turn_c + c * turn_s
            return carry

        lax.fori_loop(0, wave_rows.shape[0] // 16, fill, 0)
        south = me // half
        depth = n * PAIRS

        def add_chunk(c, first):
            own_copy(c).wait()
            each_peer(lambda peer: data_copy(c, peer, peer).wait_recv())
            parts = [[], []]
            for row in range(rows):
                source = row + south * (rows - 1 - 2 * row)
                at = pl.ds(pl.multiple_of(source * PAIRS, 8), PAIRS)
                turned = recv[c, :, at, :].reshape(depth, 4 * levels).T
                for part in range(2):
                    parts[part].append(
                        jnp.concatenate(
                            [turned[part * levels:(part + 1) * levels],
                             turned[(2 + part) * levels:(3 + part) * levels]], 1
                        )
                    )
            at = pl.ds(pl.multiple_of(c * 2 * depth, 16), 2 * depth)
            for part, total, high, low in ((0, even, cos_hi, cos_lo), (1, odd, sin_hi, sin_lo)):
                values = jnp.concatenate(parts[part], 0)
                top = values.astype(jnp.bfloat16)
                rest = (values - top.astype(jnp.float32)).astype(jnp.bfloat16)
                table = high[at, :]
                sums = jnp.dot(top, table, preferred_element_type=jnp.float32)
                sums += jnp.dot(rest, table, preferred_element_type=jnp.float32)
                sums += jnp.dot(top, low[at, :], preferred_element_type=jnp.float32)
                if first:
                    total[...] = sums
                else:
                    total[...] += sums

        add_chunk(0, True)
        if chunks > 1:
            def later(c, carry):
                add_chunk(c, False)
                return carry

            lax.fori_loop(1, chunks, later, 0)

        r = lax.broadcasted_iota(jnp.int32, (TILE, TILE), 0)
        x = lax.broadcasted_iota(jnp.int32, (TILE, TILE), 1)
        mirror = jnp.where(r + x == TILE, 1.0, 0.0).astype(jnp.bfloat16)
        at_zero = lax.broadcasted_iota(jnp.int32, (1, TILE), 1) == 0
        tiles = odd.shape[1] // TILE
        after = even[:, tiles * TILE:tiles * TILE + 1]
        for tile in range(tiles - 1, -1, -1):
            to = slice(tile * TILE, (tile + 1) * TILE)
            back = slice((2 * tiles - 1 - tile) * TILE, (2 * tiles - tile) * TILE)
            e, o = even[:, to], odd[:, to]
            out[:, :, to] = (e - o).reshape(rows, levels, TILE)
            d = e + o
            top = d.astype(jnp.bfloat16)
            rest = (d - top.astype(jnp.float32)).astype(jnp.bfloat16)
            turned = jnp.dot(top, mirror, preferred_element_type=jnp.float32)
            turned += jnp.dot(rest, mirror, preferred_element_type=jnp.float32)
            out[:, :, back] = jnp.where(at_zero, after, turned).reshape(rows, levels, TILE)
            after = d[:, 0:1]
        each_peer(lambda peer: wave_copy(peer, me).wait_send())
        for c in range(chunks):
            each_peer(lambda peer, c=c: data_copy(c, peer, me).wait_send())


def on_device(spectral, legendre, wavenumber):
    slots, degrees, _, levels = spectral.shape
    north = legendre.shape[2]
    n = lax.axis_size("wa")
    rows = 2 * north // n
    pairs = slots // 2
    real_pairs = min(pairs, PAIRS)
    chunks = pairs // real_pairs
    coeff = jnp.transpose(spectral, (0, 2, 3, 1)).reshape(slots, 2 * levels, degrees)
    values = jnp.transpose(legendre, (0, 2, 1))
    block = rows * PAIRS
    per_step = 2 * real_pairs
    depth = 2 * chunks * n * PAIRS
    middle = NLON // 2
    grid = pl.pallas_call(
        functools.partial(transform_kernel, n, chunks, real_pairs, north),
        grid=(chunks,),
        out_shape=jax.ShapeDtypeStruct((rows, levels, NLON), jnp.float32),
        in_specs=[
            pl.BlockSpec(memory_space=pltpu.SMEM),
            pl.BlockSpec((per_step, 2 * levels, degrees), lambda i: (i, 0, 0)),
            pl.BlockSpec((per_step, north, degrees), lambda i: (i, 0, 0)),
        ],
        out_specs=pl.BlockSpec(memory_space=pltpu.VMEM),
        scratch_shapes=[
            pltpu.VMEM((chunks, 2 * north * PAIRS, 4 * levels), jnp.float32),
            pltpu.VMEM((chunks, n, block, 4 * levels), jnp.float32),
            pltpu.VMEM((8, LANES), jnp.int32),
            pltpu.VMEM((n, 8, LANES), jnp.int32),
            pltpu.VMEM((LANES, LANES), jnp.float32),
            pltpu.VMEM((depth, LANES), jnp.float32),
            pltpu.VMEM((depth, middle + LANES), jnp.bfloat16),
            pltpu.VMEM((depth, middle + LANES), jnp.bfloat16),
            pltpu.VMEM((depth, middle), jnp.bfloat16),
            pltpu.VMEM((depth, middle), jnp.bfloat16),
            pltpu.VMEM((rows * levels, middle + LANES), jnp.float32),
            pltpu.VMEM((rows * levels, middle), jnp.float32),
            pltpu.SemaphoreType.DMA((chunks, n)),
            pltpu.SemaphoreType.DMA((chunks, n)),
            pltpu.SemaphoreType.DMA((n,)),
            pltpu.SemaphoreType.DMA((n,)),
            pltpu.SemaphoreType.DMA((chunks + 1,)),
        ],
        compiler_params=pltpu.CompilerParams(
            collective_id=0, has_side_effects=True, dimension_semantics=("arbitrary",)
        ),
    )(wavenumber, coeff, values)
    return jnp.transpose(grid, (0, 2, 1))


def solution(mesh):
    return jax.shard_map(
        on_device,
        mesh=mesh,
        in_specs=(P("wa", None, None, "lev"), P("wa", None, None), P("wa")),
        out_specs=P("wa", None, "lev"),
        check_vma=False,
    )
```

```python
import functools
import math

import jax
import jax.numpy as jnp
from jax import lax
from jax.experimental import pallas as pl
from jax.experimental.pallas import tpu as pltpu
from jax.sharding import PartitionSpec as P

NLON = 2560
PAIRS = 8
TILE = 256
LANES = 128


def cos_sin(turns):
    quarter = jnp.floor(turns * (4.0 / NLON) + 0.5)
    x = (turns - quarter * (NLON // 4)) * (2.0 * math.pi / NLON)
    y = x * x
    s = x * (1.0 + y * (-1 / 6 + y * (1 / 120 + y * (-1 / 5040 + y * (1 / 362880)))))
    c = 1.0 + y * (-1 / 2 + y * (1 / 24 + y * (-1 / 720 + y * (1 / 40320 - y * (1 / 3628800)))))
    which = quarter.astype(jnp.int32) & 3
    odd = (which & 1) == 1
    cos_out = jnp.where(odd, s, c)
    sin_out = jnp.where(odd, c, s)
    cos_out = jnp.where((which == 1) | (which == 2), -cos_out, cos_out)
    sin_out = jnp.where(which >= 2, -sin_out, sin_out)
    return cos_out, sin_out


def transform_kernel(
    n, chunks, real_pairs, north,
    wave_smem, spectral, legendre,
    out,
    send, recv, wave_row, wave_all, wave_columns, wave_rows,
    cos_hi, cos_lo, sin_hi, sin_lo, even, odd,
    send_sem, recv_sem, wave_send, wave_recv, own_sem,
):
    me = lax.axis_index("wa")
    step = pl.program_id(0)
    half = n // 2
    rows = 2 * north // n
    block = rows * PAIRS

    def rows_for(dst):
        south = dst // half
        slab = (1 - south) * dst + south * (half + n - 1 - dst)
        return pl.ds(pl.multiple_of(slab * block, 8), block)

    def wave_copy(peer, owner):
        return pltpu.make_async_remote_copy(
            src_ref=wave_row, dst_ref=wave_all.at[owner],
            send_sem=wave_send.at[peer], recv_sem=wave_recv.at[owner],
            device_id={"wa": peer}, device_id_type=pl.DeviceIdType.MESH,
        )

    def data_copy(c, peer, owner):
        return pltpu.make_async_remote_copy(
            src_ref=send.at[c, rows_for(peer)], dst_ref=recv.at[c, owner],
            send_sem=send_sem.at[c, peer], recv_sem=recv_sem.at[c, owner],
            device_id={"wa": peer}, device_id_type=pl.DeviceIdType.MESH,
        )

    def own_copy(c):
        return pltpu.make_async_copy(send.at[c, rows_for(me)], recv.at[c, me], own_sem.at[c])

    own_wave = pltpu.make_async_copy(wave_row, wave_all.at[me], own_sem.at[chunks])

    def each_peer(act):
        side, place = me // half, me % half

        def across(i, carry):
            act((1 - side) * half + lax.rem(place + i, half))
            return carry

        def along(i, carry):
            act(side * half + lax.rem(place + i, half))
            return carry

        lax.fori_loop(0, half, across, 0)
        lax.fori_loop(1, half, along, 0)

    @pl.when(step == 0)
    def _():
        barrier = pltpu.get_barrier_semaphore()
        each_peer(
            lambda peer: pl.semaphore_signal(
                barrier, inc=1, device_id={"wa": peer}, device_id_type=pl.DeviceIdType.MESH
            )
        )
        place = lax.broadcasted_iota(jnp.int32, wave_row.shape, 1)
        waves = jnp.zeros(wave_row.shape, jnp.int32)
        for slot in range(wave_smem.shape[0]):
            waves = jnp.where(place == slot, wave_smem[slot], waves)
        wave_row[...] = waves
        pl.semaphore_wait(barrier, n - 1)
        each_peer(lambda peer: wave_copy(peer, me).start())
        own_wave.start()

    degrees = spectral.shape[-1]
    columns = spectral.shape[1]
    levels = columns // 2
    index = lax.broadcasted_iota(jnp.int32, (1, degrees), 1)
    lane = lax.broadcasted_iota(jnp.int32, (1, 2 * columns), 1)

    def sums_of(slot):
        offset = index - wave_smem[step * 2 * real_pairs + slot]
        keep = jnp.where(offset >= 0, 1.0, 0.0)
        flip = jnp.where(offset % 2 == 0, keep, -keep)
        coeff = spectral[slot]
        both = jnp.concatenate(
            [coeff * keep.astype(coeff.dtype), coeff * flip.astype(coeff.dtype)], 0
        )
        return lax.dot_general(
            legendre[slot], both, (((1,), (1,)), ((), ())), preferred_element_type=jnp.float32
        )

    for p in range(PAIRS):
        if p < real_pairs:
            first = sums_of(2 * p)
            second = sums_of(2 * p + 1)
            first_turned = pltpu.roll(first, columns, 1)
            second_turned = pltpu.roll(second, columns, 1)
            north_rows = jnp.where(lane < columns, first, second_turned)
            south_rows = jnp.where(lane < columns, first_turned, second)
        else:
            north_rows = south_rows = jnp.zeros((north, 2 * columns), jnp.float32)
        send[step, pl.ds(p, north, stride=PAIRS), :] = north_rows
        send[step, pl.ds(north * PAIRS + p, north, stride=PAIRS), :] = south_rows

    each_peer(lambda peer: data_copy(step, peer, me).start())
    own_copy(step).start()

    @pl.when(step == chunks - 1)
    def _():
        own_wave.wait()
        each_peer(lambda peer: wave_copy(peer, peer).wait_recv())
        gathered = wave_all[:, 0, :].astype(jnp.float32)
        if n < LANES:
            gathered = jnp.concatenate([gathered, jnp.zeros((LANES - n, LANES), jnp.float32)], 0)
        wave_columns[...] = gathered.T
        for c in range(chunks):
            for sp in range(2):
                own = wave_columns[pl.ds(c * 2 * real_pairs + sp, PAIRS, stride=2), :]
                for owner in range(n):
                    to = ((2 * c + sp) * n + owner) * PAIRS
                    wave_rows[to:to + PAIRS, :] = jnp.broadcast_to(
                        own[:, owner:owner + 1], (PAIRS, LANES)
                    )
        position = lax.broadcasted_iota(jnp.int32, (1, LANES), 1).astype(jnp.float32)
        sin_tiles = sin_hi.shape[1] // LANES

        def fill(i, carry):
            at = pl.ds(pl.multiple_of(i * 16, 16), 16)
            waves = wave_rows[at, :]
            weight = jnp.where(waves == 0.0, 1.0, 2.0)
            c, s = cos_sin(waves * position)
            turn_c, turn_s = cos_sin(waves * float(LANES))
            c, s = c * weight, s * weight
            for tile in range(sin_tiles + 1):
                to = slice(tile * LANES, (tile + 1) * LANES)
                top = c.astype(jnp.bfloat16)
                cos_hi[at, to] = top
                cos_lo[at, to] = (c - top.astype(jnp.float32)).astype(jnp.bfloat16)
                if tile < sin_tiles:
                    top = s.astype(jnp.bfloat16)
                    sin_hi[at, to] = top
                    sin_lo[at, to] = (s - top.astype(jnp.float32)).astype(jnp.bfloat16)
                    c, s = c * turn_c - s * turn_s, s * turn_c + c * turn_s
            return carry

        lax.fori_loop(0, wave_rows.shape[0] // 16, fill, 0)
        south = me // half
        depth = n * PAIRS

        def add_chunk(c, first):
            own_copy(c).wait()
            each_peer(lambda peer: data_copy(c, peer, peer).wait_recv())
            parts = [[], []]
            for row in range(rows):
                source = row + south * (rows - 1 - 2 * row)
                at = pl.ds(pl.multiple_of(source * PAIRS, 8), PAIRS)
                turned = recv[c, :, at, :].reshape(depth, 4 * levels).T
                for part in range(2):
                    parts[part].append(
                        jnp.concatenate(
                            [turned[part * levels:(part + 1) * levels],
                             turned[(2 + part) * levels:(3 + part) * levels]], 1
                        )
                    )
            at = pl.ds(pl.multiple_of(c * 2 * depth, 16), 2 * depth)
            for part, total, high, low in ((0, even, cos_hi, cos_lo), (1, odd, sin_hi, sin_lo)):
                values = jnp.concatenate(parts[part], 0)
                top = values.astype(jnp.bfloat16)
                rest = (values - top.astype(jnp.float32)).astype(jnp.bfloat16)
                table = high[at, :]
                sums = jnp.dot(top, table, preferred_element_type=jnp.float32)
                sums += jnp.dot(rest, table, preferred_element_type=jnp.float32)
                sums += jnp.dot(top, low[at, :], preferred_element_type=jnp.float32)
                if first:
                    total[...] = sums
                else:
                    total[...] += sums

        add_chunk(0, True)
        if chunks > 1:
            def later(c, carry):
                add_chunk(c, False)
                return carry

            lax.fori_loop(1, chunks, later, 0)

        r = lax.broadcasted_iota(jnp.int32, (TILE, TILE), 0)
        x = lax.broadcasted_iota(jnp.int32, (TILE, TILE), 1)
        mirror = jnp.where(r + x == TILE, 1.0, 0.0).astype(jnp.bfloat16)
        at_zero = lax.broadcasted_iota(jnp.int32, (1, TILE), 1) == 0
        tiles = odd.shape[1] // TILE
        after = even[:, tiles * TILE:tiles * TILE + 1]
        for tile in range(tiles - 1, -1, -1):
            to = slice(tile * TILE, (tile + 1) * TILE)
            back = slice((2 * tiles - 1 - tile) * TILE, (2 * tiles - tile) * TILE)
            e, o = even[:, to], odd[:, to]
            out[:, :, to] = (e - o).reshape(rows, levels, TILE)
            d = e + o
            top = d.astype(jnp.bfloat16)
            rest = (d - top.astype(jnp.float32)).astype(jnp.bfloat16)
            turned = jnp.dot(top, mirror, preferred_element_type=jnp.float32)
            turned += jnp.dot(rest, mirror, preferred_element_type=jnp.float32)
            out[:, :, back] = jnp.where(at_zero, after, turned).reshape(rows, levels, TILE)
            after = d[:, 0:1]
        each_peer(lambda peer: wave_copy(peer, me).wait_send())
        for c in range(chunks):
            each_peer(lambda peer, c=c: data_copy(c, peer, me).wait_send())


def on_device(spectral, legendre, wavenumber):
    slots, degrees, _, levels = spectral.shape
    north = legendre.shape[2]
    n = lax.axis_size("wa")
    rows = 2 * north // n
    pairs = slots // 2
    real_pairs = min(pairs, PAIRS)
    chunks = pairs // real_pairs
    coeff = jnp.transpose(spectral, (0, 2, 3, 1)).reshape(slots, 2 * levels, degrees)
    values = jnp.transpose(legendre, (0, 2, 1))
    block = rows * PAIRS
    per_step = 2 * real_pairs
    depth = 2 * chunks * n * PAIRS
    middle = NLON // 2
    grid = pl.pallas_call(
        functools.partial(transform_kernel, n, chunks, real_pairs, north),
        grid=(chunks,),
        out_shape=jax.ShapeDtypeStruct((rows, levels, NLON), jnp.float32),
        in_specs=[
            pl.BlockSpec(memory_space=pltpu.SMEM),
            pl.BlockSpec((per_step, 2 * levels, degrees), lambda i: (i, 0, 0)),
            pl.BlockSpec((per_step, north, degrees), lambda i: (i, 0, 0)),
        ],
        out_specs=pl.BlockSpec(memory_space=pltpu.VMEM),
        scratch_shapes=[
            pltpu.VMEM((chunks, 2 * north * PAIRS, 4 * levels), jnp.float32),
            pltpu.VMEM((chunks, n, block, 4 * levels), jnp.float32),
            pltpu.VMEM((8, LANES), jnp.int32),
            pltpu.VMEM((n, 8, LANES), jnp.int32),
            pltpu.VMEM((LANES, LANES), jnp.float32),
            pltpu.VMEM((depth, LANES), jnp.float32),
            pltpu.VMEM((depth, middle + LANES), jnp.bfloat16),
            pltpu.VMEM((depth, middle + LANES), jnp.bfloat16),
            pltpu.VMEM((depth, middle), jnp.bfloat16),
            pltpu.VMEM((depth, middle), jnp.bfloat16),
            pltpu.VMEM((rows * levels, middle + LANES), jnp.float32),
            pltpu.VMEM((rows * levels, middle), jnp.float32),
            pltpu.SemaphoreType.DMA((chunks, n)),
            pltpu.SemaphoreType.DMA((chunks, n)),
            pltpu.SemaphoreType.DMA((n,)),
            pltpu.SemaphoreType.DMA((n,)),
            pltpu.SemaphoreType.DMA((chunks + 1,)),
        ],
        compiler_params=pltpu.CompilerParams(
            collective_id=0, has_side_effects=True, dimension_semantics=("arbitrary",),
            vmem_limit_bytes=48 * 2**20,
        ),
    )(wavenumber, coeff, values)
    return jnp.transpose(grid, (0, 2, 1))


def solution(mesh):
    return jax.shard_map(
        on_device,
        mesh=mesh,
        in_specs=(P("wa", None, None, "lev"), P("wa", None, None), P("wa")),
        out_specs=P("wa", None, "lev"),
        check_vma=False,
    )
```
